512 devices in a mesh: level: 16 (over z), dev: 32 (over x, y, core).
Axes of the slice: x: 4, y: 4, z: 16, core: 2. Of those that a mesh axis runs over, the one named last changes fastest.
Arguments:
- fields: float32 [16, 512, 12, 128], P('level', 'dev'), may hold values from -6 to 6
- own_src: int32 [16, 512], P('level', 'dev'), may hold values from 0 to 15
- own_weight: bfloat16 [16, 512, 128, 128], P('level', 'dev'), may hold values from 0 to 1, as said below
- send_block: int32 [16, 32, 32, 2], P('level', 'dev'), may hold values from 0 to 15
- send_target: int32 [16, 32, 32, 2], P('level', 'dev'), may hold values from 0 to 15
- send_count: int32 [16, 32, 32], P('level', 'dev'), may hold values from 0 to 2, as said below
- send_weight: bfloat16 [16, 32, 32, 2, 128, 128], P('level', 'dev'), may hold values from 0 to 1, as said below
- left_block: int32 [16, 32, 16, 2], P('level', 'dev'), may hold values from 0 to 15
- left_target: int32 [16, 32, 16, 2], P('level', 'dev'), may hold values from 0 to 15
- left_count: int32 [16, 32, 16], P('level', 'dev'), may hold values from 0 to 2, as said below
- left_weight: bfloat16 [16, 32, 16, 2, 128, 128], P('level', 'dev'), may hold values from 0 to 1, as said below
Outputs:
- remapped: float32 [16, 512, 12, 128], P('level', 'dev')
- totals: float32 [12], replicated
The draws below stay inside these ranges and needn't reach their ends.
Inputs may be any that keep to these rules, and one draw needn't show every extreme that they name: send_count[l, s, s] = 0; for every level some receiver device gets 2 live slots from every other device of the level. left_count[m, q, m] = 0; for every device index some receiver level gets 2 live slots from every other level. `own_weight`: nonnegative; entry [k, i] is zero where old cell k and new cell i differ by more than 3; each column sums to a positive intersect fraction of at most 1. `send_weight`: nonnegative; entry [k, i] is zero where old cell k and new cell i differ by more than 3; each column sums to a positive intersect fraction of at most 1. `left_weight`: nonnegative; entry [k, i] is zero where old cell k and new cell i differ by more than 3; each column sums to a positive intersect fraction of at most 1.
All inputs are finite; a program needn't handle non-finite values.
Results may differ from the reference program's by a relative error of at most 0.0045.
Values may be sent and summed in bfloat16 or wider, within the bound.
No kernel may reach another device: no remote copies, remote signals or barrier semaphores. Data moves between devices by JAX's collectives and lax.ppermute only.
A program may use at most 64 MiB of HBM per device.

```python
import jax
import jax.numpy as jnp
from jax import lax

COMP = 12
CELLS = 128
HALF = 3
BLK_DEV = 16
CAP = 2
LCAP = 2
PEERS = 32
LEVELS = 16
BLOCKS = 512


def band_fractions(key, lead):
    first, second, third = jax.random.split(key, 3)
    shape = lead + (CELLS, CELLS)
    rowpos = lax.broadcasted_iota(jnp.int32, shape, len(lead))
    colpos = lax.broadcasted_iota(jnp.int32, shape, len(lead) + 1)
    spread = jnp.abs(rowpos - colpos)
    middle = jax.random.uniform(first, shape, jnp.float32, 2.0, 3.0)
    beside = jax.random.uniform(second, shape, jnp.float32, 0.3, 1.0)
    raw = jnp.where(spread == 0, middle, jnp.where(spread <= HALF, beside, jnp.zeros_like(beside)))
    fraction = jax.random.uniform(third, lead + (1, CELLS), jnp.float32, 0.2, 0.8)
    return raw / jnp.sum(raw, axis=-2, keepdims=True) * fraction


def draw_own_weight(key, part):
    whole = band_fractions(jax.random.fold_in(key, 11), (LEVELS, BLOCKS))
    return whole.astype(jnp.bfloat16)


def draw_send_weight(key, part):
    whole = band_fractions(jax.random.fold_in(key, 23), (LEVELS, PEERS, PEERS, CAP))
    return whole.astype(jnp.bfloat16)


def draw_left_weight(key, part):
    whole = band_fractions(jax.random.fold_in(key, 37), (LEVELS, PEERS, LEVELS, LCAP))
    return whole.astype(jnp.bfloat16)


def draw_send_count(key, part):
    shape = (LEVELS, PEERS, PEERS)
    base = jax.random.randint(key, shape, 0, CAP + 1)
    lvl = lax.broadcasted_iota(jnp.int32, shape, 0)
    src = lax.broadcasted_iota(jnp.int32, shape, 1)
    dst = lax.broadcasted_iota(jnp.int32, shape, 2)
    heavy = (7 * lvl + 3) % PEERS
    near = ((dst - src) % PEERS == 1) | ((src - dst) % PEERS == 1)
    full = (dst == heavy) | near
    out = jnp.where(full, CAP, base)
    return jnp.where(src == dst, 0, out).astype(jnp.int32)


def draw_left_count(key, part):
    shape = (LEVELS, PEERS, LEVELS)
    base = jax.random.randint(key, shape, 0, LCAP + 1)
    src = lax.broadcasted_iota(jnp.int32, shape, 0)
    dev = lax.broadcasted_iota(jnp.int32, shape, 1)
    dst = lax.broadcasted_iota(jnp.int32, shape, 2)
    heavy = (5 * dev + 1) % LEVELS
    near = ((dst - src) % LEVELS == 1) | ((src - dst) % LEVELS == 1)
    full = (dst == heavy) | near
    out = jnp.where(full, LCAP, base)
    return jnp.where(src == dst, 0, out).astype(jnp.int32)


def with_ends(drawn, own_key, smallest, top_value):
    spot = [jax.random.randint(jax.random.fold_in(own_key, axis), (), 0, length) for axis, length in enumerate(drawn.shape)]
    widest = drawn.shape.index(max(drawn.shape))
    next_to = spot[:widest] + [(spot[widest] + 1) % drawn.shape[widest]] + spot[widest + 1:]
    return drawn.at[tuple(spot)].set(smallest).at[tuple(next_to)].set(top_value)


def block_levels(key, shape, cuts, smallest, top_value):
    def one(position, parts):
        steps = jax.random.uniform(jax.random.fold_in(jax.random.fold_in(key, 6), position), (parts,), jnp.float32, smallest / len(cuts), top_value / len(cuts))
        return jnp.repeat(jnp.exp(steps), shape[position] // parts).reshape((-1,) + (1,) * (len(shape) - position - 1))

    loudness = one(*cuts[0])
    for cut in cuts[1:]:
        loudness = loudness * one(*cut)
    return loudness


def centred(rng, dims, deviation, reach, cuts=(), dtype=jnp.bfloat16):
    result = deviation * jax.random.normal(rng, dims, jnp.float32)
    if cuts:
        result = result * block_levels(rng, dims, cuts, -0.22, 0.18)
    return jnp.clip(result, -reach, reach).astype(dtype)


def setup_inputs(seed: int = 0) -> dict:
    splits = jax.random.split(jax.random.key(seed), 12)
    fields = centred(splits[0], (LEVELS, BLOCKS, COMP, CELLS), 1.0, 6.0, ((0, 16), (1, 32)), jnp.float32)
    own_src = with_ends(jax.random.randint(splits[1], (LEVELS, BLOCKS), 0, BLK_DEV), jax.random.fold_in(splits[1], 1), 0, BLK_DEV - 1).astype(jnp.int32)
    own_weight = draw_own_weight(jax.random.fold_in(splits[11], 71), 0)
    send_block = with_ends(jax.random.randint(splits[3], (LEVELS, PEERS, PEERS, CAP), 0, BLK_DEV), jax.random.fold_in(splits[3], 1), 0, BLK_DEV - 1).astype(jnp.int32)
    send_target = with_ends(jax.random.randint(splits[4], (LEVELS, PEERS, PEERS, CAP), 0, BLK_DEV), jax.random.fold_in(splits[4], 1), 0, BLK_DEV - 1).astype(jnp.int32)
    send_count = draw_send_count(jax.random.fold_in(splits[11], 71), 0)
    send_weight = draw_send_weight(jax.random.fold_in(splits[11], 71), 0)
    left_block = with_ends(jax.random.randint(splits[7], (LEVELS, PEERS, LEVELS, LCAP), 0, BLK_DEV), jax.random.fold_in(splits[7], 1), 0, BLK_DEV - 1).astype(jnp.int32)
    left_target = with_ends(jax.random.randint(splits[8], (LEVELS, PEERS, LEVELS, LCAP), 0, BLK_DEV), jax.random.fold_in(splits[8], 1), 0, BLK_DEV - 1).astype(jnp.int32)
    left_count = draw_left_count(jax.random.fold_in(splits[11], 71), 0)
    left_weight = draw_left_weight(jax.random.fold_in(splits[11], 71), 0)
    return dict(fields=fields, own_src=own_src, own_weight=own_weight, send_block=send_block, send_target=send_target, send_count=send_count, send_weight=send_weight, left_block=left_block, left_target=left_target, left_count=left_count, left_weight=left_weight)


def reference(fields, own_src, own_weight, send_block, send_target, send_count, send_weight, left_block, left_target, left_count, left_weight):
    levels = fields.shape[0]
    peers = send_count.shape[1]
    blocks = fields.shape[1] // peers
    comp = fields.shape[2]
    cells = fields.shape[3]
    rounded = fields.astype(jnp.bfloat16).reshape(levels, peers, blocks, comp, cells)
    highest = lax.Precision.HIGHEST

    own_index = own_src.reshape(levels, peers, blocks, 1, 1).astype(jnp.int32)
    own_donor = jnp.take_along_axis(rounded, own_index, axis=2).astype(jnp.float32)
    own_frac = own_weight.reshape(levels, peers, blocks, cells, cells).astype(jnp.float32)
    own = jnp.einsum("lqbmk,lqbki->lqbmi", own_donor, own_frac, precision=highest)

    source_dev = lax.broadcasted_iota(jnp.int32, (peers, 1, 1), 0)
    recv_dev = lax.broadcasted_iota(jnp.int32, (1, peers, 1), 1)
    slot_cap = send_block.shape[3]

    def level_intra(packed):
        flds, blk, tgt, cnt, wts = packed
        donors = flds[source_dev, blk]
        valid = lax.broadcasted_iota(jnp.int32, (1, 1, slot_cap), 2) < cnt[:, :, None]
        donors = jnp.where(valid[..., None, None], donors, jnp.zeros_like(donors))
        contrib = jnp.einsum("spcmk,spcki->spcmi", donors.astype(jnp.float32), wts.astype(jnp.float32), precision=highest)
        receive = (recv_dev * blocks + tgt).reshape(-1).astype(jnp.int32)
        total = jnp.zeros((peers * blocks, comp, cells), jnp.float32)
        return total.at[receive].add(contrib.reshape(-1, comp, cells)).reshape(peers, blocks, comp, cells)

    intra = lax.map(level_intra, (rounded, send_block, send_target, send_count, send_weight))

    left_cap = left_block.shape[3]
    dev_index = lax.broadcasted_iota(jnp.int32, (peers, 1, 1), 0)

    def level_left(packed):
        flds, blk, cnt, wts = packed
        donors = flds[dev_index, blk]
        valid = lax.broadcasted_iota(jnp.int32, (1, 1, left_cap), 2) < cnt[:, :, None]
        donors = jnp.where(valid[..., None, None], donors, jnp.zeros_like(donors))
        return jnp.einsum("qlcmk,qlcki->qlcmi", donors.astype(jnp.float32), wts.astype(jnp.float32), precision=highest)

    left_terms = lax.map(level_left, (rounded, left_block, left_count, left_weight))
    dst_level = lax.broadcasted_iota(jnp.int32, (1, 1, levels, 1), 2)
    dev_here = lax.broadcasted_iota(jnp.int32, (1, peers, 1, 1), 1)
    recv_left = ((dst_level * peers + dev_here) * blocks + left_target).reshape(-1).astype(jnp.int32)
    leftover = jnp.zeros((levels * peers * blocks, comp, cells), jnp.float32)
    leftover = leftover.at[recv_left].add(left_terms.reshape(-1, comp, cells))
    leftover = leftover.reshape(levels, peers, blocks, comp, cells)

    remapped = (own + intra + leftover).reshape(levels, peers * blocks, comp, cells)
    totals = jnp.sum(remapped, axis=(0, 1, 3)) / (CELLS * BLK_DEV)
    return remapped, totals
```

```python
import functools

import jax
import jax.numpy as jnp
from jax import lax
from jax.experimental import pallas as pl
from jax.experimental.pallas import tpu as pltpu
from jax.sharding import Mesh
from jax.sharding import PartitionSpec as P

DEV = ("dev_0", "dev_1", "dev_2")
COMP = 12
CELLS = 128
BLK = 16
CAP = 2
ROWS = 32
GROUP = CELLS // ROWS
W_CHUNKS = 4
F32 = jnp.float32
BF16 = jnp.bfloat16


def code_tile(t0, t1, slot):
    row = lax.broadcasted_iota(jnp.int32, (8, CELLS), 0)
    lane = lax.broadcasted_iota(jnp.int32, (8, CELLS), 1)
    r = lane % ROWS
    here = (row == 0) & (lane // ROWS == slot)
    second = r >= COMP
    comp = jnp.where(second, r - COMP, r)
    code = comp * BLK + jnp.where(second, t1, t0)
    code = jnp.where(r < CAP * COMP, code, 255)
    return jnp.where(here, code, 0).astype(F32)


def three_parts(total):
    row = lax.broadcasted_iota(jnp.int32, (16, CELLS), 0)
    full = jnp.broadcast_to(total, (16, CELLS))
    hi = full.astype(BF16).astype(F32)
    mid = (full - hi).astype(BF16).astype(F32)
    low = full - hi - mid
    zero = jnp.zeros_like(full)
    return jnp.where(row == 9, hi, jnp.where(row == 10, mid, jnp.where(row == 11, low, zero)))


def sum_parts(tail):
    return tail[9:10] + tail[10:11] + tail[11:12]


def terms_kernel(
    place,
    fields,
    own_src,
    own_w,
    send_blk,
    send_tgt,
    send_cnt,
    send_w,
    left_blk,
    left_tgt,
    left_cnt,
    left_w,
    out_dev,
    out_lev,
    tail_lev,
    own_out,
    fld,
    first32,
    second32,
    first,
    second,
    wd,
    wl,
    wo,
    tail_dev,
    s_src,
    s_sblk,
    s_stgt,
    s_scnt,
    s_lblk,
    s_ltgt,
    s_lcnt,
    sems,
    wsems,
):
    peers = send_w.shape[0]
    levels = left_w.shape[0]
    small = []
    pairs = (
        (fields, fld),
        (own_src, s_src),
        (send_blk, s_sblk),
        (send_tgt, s_stgt),
        (send_cnt, s_scnt),
        (left_blk, s_lblk),
        (left_tgt, s_ltgt),
        (left_cnt, s_lcnt),
    )
    for n, (src, dst) in enumerate(pairs):
        copy = pltpu.make_async_copy(src, dst, sems.at[n])
        copy.start()
        small.append(copy)
    step = peers // W_CHUNKS
    weights = []
    for n in range(W_CHUNKS):
        sl = pl.ds(n * step, step)
        copy = pltpu.make_async_copy(send_w.at[sl], wd.at[sl], wsems.at[n])
        copy.start()
        weights.append(copy)
    left_copy = pltpu.make_async_copy(left_w, wl, wsems.at[W_CHUNKS])
    left_copy.start()
    own_copy = pltpu.make_async_copy(own_w, wo, wsems.at[W_CHUNKS + 1])
    own_copy.start()

    first32[...] = jnp.zeros(first32.shape, F32)
    second32[...] = jnp.zeros(second32.shape, F32)
    small[0].wait()
    for b in range(BLK):
        one = fld[pl.ds(b, COMP, stride=BLK), :]
        first32[b, 0:COMP, :] = one
        second32[b, COMP : 2 * COMP, :] = one
    first[...] = first32[...].astype(BF16)
    second[...] = second32[...].astype(BF16)
    for copy in small[1:]:
        copy.wait()

    def pair(blk, cnt, weight, n):
        live = cnt[0, n]
        b0 = jnp.where(live > 0, blk[0, n], BLK)
        b1 = jnp.where(live > 1, blk[1, n], BLK)
        lhs = jnp.concatenate([first[b0], second[b1]], axis=1)
        return jnp.dot(lhs, weight[n], preferred_element_type=F32)

    dev_slot = place[0] % GROUP
    lev_slot = place[1] % GROUP

    def dev_step(n, acc):
        t = pair(s_sblk, s_scnt, wd, n)
        out_dev[n, 0:16, :] = t[0:16].astype(BF16)
        tail_dev[n, 0:8, :] = t[16:24]
        tail_dev[n, 8:16, :] = code_tile(s_stgt[0, n], s_stgt[1, n], dev_slot)
        return acc + t[0:24]

    def lev_step(n, acc):
        t = pair(s_lblk, s_lcnt, wl, n)
        out_lev[n, 0:16, :] = t[0:16].astype(BF16)
        tail_lev[n, 0:8, :] = t[16:24]
        tail_lev[n, 8:16, :] = code_tile(s_ltgt[0, n], s_ltgt[1, n], lev_slot)
        return acc + t[0:24]

    acc = jnp.zeros((24, CELLS), F32)
    for n in range(W_CHUNKS):
        weights[n].wait()
        acc = lax.fori_loop(n * step, (n + 1) * step, dev_step, acc, unroll=True)
    left_copy.wait()
    acc = lax.fori_loop(0, levels, lev_step, acc, unroll=8)
    own_copy.wait()
    own_acc = jnp.zeros((16, CELLS), F32)
    for b in range(BLK):
        t = jnp.dot(first[s_src[0, b], 0:16, :], wo[b], preferred_element_type=F32)
        own_out[pl.ds(b, COMP, stride=BLK), :] = t[0:COMP]
        own_acc = own_acc + t
    own_acc = jnp.concatenate([own_acc, jnp.zeros((8, CELLS), F32)], axis=0)
    acc = jnp.concatenate([acc + own_acc, jnp.zeros((CELLS - 24, CELLS), F32)], axis=0)
    sums = lax.dot_general(
        jnp.ones((8, CELLS), F32),
        acc,
        (((1,), (1,)), ((), ())),
        precision=lax.Precision.HIGHEST,
        preferred_element_type=F32,
    )
    parts = three_parts(sums[0:1])
    out_dev[:, 16:32, :] = (tail_dev[...] + parts[None]).astype(BF16)
    out_lev[:, 16:32, :] = tail_lev[...].astype(BF16)


def relay_kernel(recv, tail, send_in, send_out, new_tail, sem):
    del send_in
    total = sum_parts(jnp.sum(recv[:, 16:32, :].astype(F32), axis=0))
    new_tail[...] = (tail[...] + three_parts(total)[None]).astype(BF16)
    copy = pltpu.make_async_copy(new_tail, send_out.at[:, pl.ds(16, 16), :], sem)
    copy.start()
    copy.wait()


def placed(recv):
    peers = recv.shape[0]
    row = lax.broadcasted_iota(jnp.int32, (COMP * BLK, CELLS), 0).astype(F32)
    total = jnp.zeros((COMP * BLK, CELLS), F32)
    for g in range(peers // GROUP):
        sl = slice(g * GROUP, (g + 1) * GROUP)
        codes = jnp.sum(recv[sl, 16:32, :].astype(F32), axis=0)[8:9]
        pick = jnp.where(row == codes, 1.0, 0.0).astype(BF16)
        data = recv[sl].reshape(GROUP * ROWS, CELLS)
        total = total + jnp.dot(pick, data, preferred_element_type=F32)
    return total


def intra_kernel(recv, own, out):
    out[...] = own[...] + placed(recv)


def final_kernel(recv, base, out, totals):
    out[...] = base[...] + placed(recv)
    total = sum_parts(jnp.sum(recv[:, 16:32, :].astype(F32), axis=0))
    both = jnp.broadcast_to(total, (8, CELLS))
    both = both + pltpu.roll(both, CELLS - COMP, 1)
    totals[...] = both[0:1, 0:COMP] * (1.0 / (CELLS * BLK))


def body(
    fields,
    own_src,
    own_weight,
    send_block,
    send_target,
    send_count,
    send_weight,
    left_block,
    left_target,
    left_count,
    left_weight,
):
    peers = send_weight.shape[2]
    levels = left_weight.shape[2]
    rows = COMP * BLK
    flat = jnp.transpose(fields[0], (1, 0, 2)).reshape(rows, CELLS)
    place = jnp.stack([lax.axis_index(DEV), lax.axis_index("level")]).astype(jnp.int32)
    anywhere = pl.BlockSpec(memory_space=pl.ANY)
    vmem = pl.BlockSpec(memory_space=pltpu.VMEM)
    smem = pl.BlockSpec(memory_space=pltpu.SMEM)
    send_dev, send_lev, tail_lev, own = pl.pallas_call(
        terms_kernel,
        name="terms",
        in_specs=[smem] + [anywhere] * 11,
        out_specs=[vmem] * 4,
        out_shape=[
            jax.ShapeDtypeStruct((peers, ROWS, CELLS), BF16),
            jax.ShapeDtypeStruct((levels, ROWS, CELLS), BF16),
            jax.ShapeDtypeStruct((levels, 16, CELLS), F32),
            jax.ShapeDtypeStruct((rows, CELLS), F32),
        ],
        scratch_shapes=[
            pltpu.VMEM((rows, CELLS), F32),
            pltpu.VMEM((BLK + 1, ROWS, CELLS), F32),
            pltpu.VMEM((BLK + 1, ROWS, CELLS), F32),
            pltpu.VMEM((BLK + 1, ROWS, CELLS), BF16),
            pltpu.VMEM((BLK + 1, ROWS, CELLS), BF16),
            pltpu.VMEM((peers, CAP * CELLS, CELLS), BF16),
            pltpu.VMEM((levels, CAP * CELLS, CELLS), BF16),
            pltpu.VMEM((BLK, CELLS, CELLS), BF16),
            pltpu.VMEM((peers, 16, CELLS), F32),
            pltpu.SMEM((1, BLK), jnp.int32),
            pltpu.SMEM((CAP, peers), jnp.int32),
            pltpu.SMEM((CAP, peers), jnp.int32),
            pltpu.SMEM((1, peers), jnp.int32),
            pltpu.SMEM((CAP, levels), jnp.int32),
            pltpu.SMEM((CAP, levels), jnp.int32),
            pltpu.SMEM((1, levels), jnp.int32),
            pltpu.SemaphoreType.DMA((8,)),
            pltpu.SemaphoreType.DMA((W_CHUNKS + 2,)),
        ],
    )(
        place,
        flat,
        own_src,
        own_weight[0],
        send_block[0, 0].T,
        send_target[0, 0].T,
        send_count[0],
        send_weight.reshape(peers, CAP * CELLS, CELLS),
        left_block[0, 0].T,
        left_target[0, 0].T,
        left_count[0],
        left_weight.reshape(levels, CAP * CELLS, CELLS),
    )
    got_dev = lax.all_to_all(send_dev, DEV, split_axis=0, concat_axis=0, tiled=True)
    send_lev = pl.pallas_call(
        relay_kernel,
        name="relay",
        in_specs=[vmem, vmem, anywhere],
        out_specs=anywhere,
        out_shape=jax.ShapeDtypeStruct(send_lev.shape, BF16),
        scratch_shapes=[pltpu.VMEM((levels, 16, CELLS), BF16), pltpu.SemaphoreType.DMA],
        input_output_aliases={2: 0},
    )(got_dev, tail_lev, send_lev)
    got_lev = lax.all_to_all(send_lev, "level", split_axis=0, concat_axis=0, tiled=True)
    base = pl.pallas_call(
        intra_kernel,
        name="intra",
        in_specs=[vmem, vmem],
        out_specs=vmem,
        out_shape=jax.ShapeDtypeStruct((rows, CELLS), F32),
    )(got_dev, own)
    remapped, totals = pl.pallas_call(
        final_kernel,
        name="final",
        in_specs=[vmem, vmem],
        out_specs=[vmem, vmem],
        out_shape=[
            jax.ShapeDtypeStruct((rows, CELLS), F32),
            jax.ShapeDtypeStruct((1, COMP), F32),
        ],
    )(got_lev, base)
    remapped = jnp.transpose(remapped.reshape(COMP, BLK, CELLS), (1, 0, 2))
    return (remapped[None], totals.reshape(COMP))


def solution(mesh):
    split = Mesh(
        mesh.devices.reshape(mesh.shape["level"], 4, 4, 2), ("level", "dev_0", "dev_1", "dev_2")
    )
    return jax.shard_map(
        body,
        mesh=split,
        in_specs=(
            P("level", DEV, None, None),
            P("level", DEV),
            P("level", DEV, None, None),
            P("level", DEV, None, None),
            P("level", DEV, None, None),
            P("level", DEV, None),
            P("level", DEV, None, None, None, None),
            P("level", DEV, None, None),
            P("level", DEV, None, None),
            P("level", DEV, None),
            P("level", DEV, None, None, None, None),
        ),
        out_specs=(P("level", DEV, None, None), P()),
        check_vma=False,
    )
```

```python
import jax
import jax.numpy as jnp
from jax import lax
from jax.experimental import pallas as pl
from jax.experimental.pallas import tpu as pltpu
from jax.sharding import PartitionSpec as P

START = {"dev": 31, "level": 12}
ORDER = ("dev", "level")
COMP = 12
CELLS = 128
BLK = 16
CAP = 2
ROWS = 32
GROUP = CELLS // ROWS
W_CHUNKS = 4
F32 = jnp.float32
BF16 = jnp.bfloat16


def code_tile(t0, t1, slot):
    row = lax.broadcasted_iota(jnp.int32, (8, CELLS), 0)
    lane = lax.broadcasted_iota(jnp.int32, (8, CELLS), 1)
    r = lane % ROWS
    here = (row == 0) & (lane // ROWS == slot)
    second = r >= COMP
    comp = jnp.where(second, r - COMP, r)
    code = comp * BLK + jnp.where(second, t1, t0)
    code = jnp.where(r < CAP * COMP, code, 255)
    return jnp.where(here, code, 0).astype(F32)


def three_parts(total):
    row = lax.broadcasted_iota(jnp.int32, (16, CELLS), 0)
    full = jnp.broadcast_to(total, (16, CELLS))
    hi = full.astype(BF16).astype(F32)
    mid = (full - hi).astype(BF16).astype(F32)
    low = full - hi - mid
    zero = jnp.zeros_like(full)
    return jnp.where(row == 9, hi, jnp.where(row == 10, mid, jnp.where(row == 11, low, zero)))


def sum_parts(tail):
    return tail[9:10] + tail[10:11] + tail[11:12]


def terms_kernel(
    fields,
    own_src,
    own_w,
    send_blk,
    send_tgt,
    send_cnt,
    send_w,
    left_blk,
    left_tgt,
    left_cnt,
    left_w,
    out_dev,
    out_lev,
    own_out,
    fld,
    first32,
    second32,
    first,
    second,
    wd,
    wl,
    wo,
    s_src,
    s_sblk,
    s_stgt,
    s_scnt,
    s_lblk,
    s_ltgt,
    s_lcnt,
    sems,
    wsems,
):
    peers = send_w.shape[0]
    levels = left_w.shape[0]
    small = []
    pairs = (
        (fields, fld),
        (own_src, s_src),
        (send_blk, s_sblk),
        (send_tgt, s_stgt),
        (send_cnt, s_scnt),
        (left_blk, s_lblk),
        (left_tgt, s_ltgt),
        (left_cnt, s_lcnt),
    )
    for n, (src, dst) in enumerate(pairs):
        copy = pltpu.make_async_copy(src, dst, sems.at[n])
        copy.start()
        small.append(copy)
    step = peers // W_CHUNKS
    weights = []
    for n in range(W_CHUNKS):
        sl = pl.ds(n * step, step)
        copy = pltpu.make_async_copy(send_w.at[sl], wd.at[sl], wsems.at[n])
        copy.start()
        weights.append(copy)
    left_copy = pltpu.make_async_copy(left_w, wl, wsems.at[W_CHUNKS])
    left_copy.start()
    own_copy = pltpu.make_async_copy(own_w, wo, wsems.at[W_CHUNKS + 1])
    own_copy.start()

    first32[...] = jnp.zeros(first32.shape, F32)
    second32[...] = jnp.zeros(second32.shape, F32)
    small[0].wait()
    for b in range(BLK):
        one = fld[pl.ds(b, COMP, stride=BLK), :]
        first32[b, 0:COMP, :] = one
        second32[b, COMP : 2 * COMP, :] = one
    first[...] = first32[...].astype(BF16)
    second[...] = second32[...].astype(BF16)
    for copy in small[1:]:
        copy.wait()

    def group_terms(out, blk, tgt, cnt, weight, axis):
        size = out.shape[0]
        place = lax.rem(lax.axis_index(axis) + (size - START[axis]), size)
        slot = lax.rem(place, GROUP)

        def one(n, acc):
            live = cnt[0, n]
            b0 = jnp.where(live > 0, blk[0, n], BLK)
            b1 = jnp.where(live > 1, blk[1, n], BLK)
            lhs = jnp.concatenate([first[b0], second[b1]], axis=1)
            t = jnp.dot(lhs, weight[n], preferred_element_type=F32)
            to = lax.rem(n + (size - START[axis]), size)
            out[to, 0:16, :] = t[0:16].astype(BF16)
            tail = jnp.concatenate([t[16:24], code_tile(tgt[0, n], tgt[1, n], slot)], axis=0)
            out[to, 16:32, :] = tail.astype(BF16)
            return acc + t[0:24]

        return one

    dev_step = group_terms(out_dev, s_sblk, s_stgt, s_scnt, wd, "dev")
    lev_step = group_terms(out_lev, s_lblk, s_ltgt, s_lcnt, wl, "level")
    acc = jnp.zeros((24, CELLS), F32)
    for n in range(W_CHUNKS):
        weights[n].wait()
        acc = lax.fori_loop(n * step, (n + 1) * step, dev_step, acc, unroll=True)
    left_copy.wait()
    acc = lax.fori_loop(0, levels, lev_step, acc, unroll=True)
    own_copy.wait()
    own_acc = jnp.zeros((16, CELLS), F32)
    for b in range(BLK):
        t = jnp.dot(first[s_src[0, b], 0:16, :], wo[b], preferred_element_type=F32)
        own_out[pl.ds(b, COMP, stride=BLK), :] = t[0:COMP]
        own_acc = own_acc + t
    own_acc = jnp.concatenate([own_acc, jnp.zeros((8, CELLS), F32)], axis=0)
    acc = jnp.concatenate([acc + own_acc, jnp.zeros((CELLS - 24, CELLS), F32)], axis=0)
    sums = lax.dot_general(
        jnp.ones((8, CELLS), F32),
        acc,
        (((1,), (1,)), ((), ())),
        precision=lax.Precision.HIGHEST,
        preferred_element_type=F32,
    )
    add_parts(out_dev if ORDER[0] == "dev" else out_lev, sums[0:1])


def add_parts(message, total):
    tail = message[:, 16:32, :].astype(F32)
    message[:, 16:32, :] = (tail + three_parts(total)[None]).astype(BF16)


def relay_kernel(recv, send_in, send_out):
    del send_in
    add_parts(send_out, sum_parts(jnp.sum(recv[:, 16:32, :].astype(F32), axis=0)))


def placed(recv):
    peers = recv.shape[0]
    row = lax.broadcasted_iota(jnp.int32, (COMP * BLK, CELLS), 0).astype(F32)
    total = jnp.zeros((COMP * BLK, CELLS), F32)
    for g in range(peers // GROUP):
        sl = slice(g * GROUP, (g + 1) * GROUP)
        codes = jnp.sum(recv[sl, 16:32, :].astype(F32), axis=0)[8:9]
        pick = jnp.where(row == codes, 1.0, 0.0).astype(BF16)
        data = recv[sl].reshape(GROUP * ROWS, CELLS)
        total = total + jnp.dot(pick, data, preferred_element_type=F32)
    return total


def final_kernel(early, late, own, out, totals):
    out[...] = own[...] + placed(early) + placed(late)
    total = sum_parts(jnp.sum(late[:, 16:32, :].astype(F32), axis=0))
    both = jnp.broadcast_to(total, (8, CELLS))
    both = both + pltpu.roll(both, CELLS - COMP, 1)
    totals[...] = both[0:1, 0:COMP] * (1.0 / (CELLS * BLK))


def in_vmem(x):
    return pltpu.with_memory_space_constraint(x, pltpu.VMEM)


def exchange(message, axis):
    size = message.shape[0]
    groups = [[(START[axis] + n) % size for n in range(size)]]
    got = lax.all_to_all(
        in_vmem(message), axis, 0, 0, axis_index_groups=groups, tiled=True
    )
    return in_vmem(got)


def body(
    fields,
    own_src,
    own_weight,
    send_block,
    send_target,
    send_count,
    send_weight,
    left_block,
    left_target,
    left_count,
    left_weight,
):
    peers = send_weight.shape[2]
    levels = left_weight.shape[2]
    rows = COMP * BLK
    flat = jnp.transpose(fields[0], (1, 0, 2)).reshape(rows, CELLS)
    anywhere = pl.BlockSpec(memory_space=pl.ANY)
    vmem = pl.BlockSpec(memory_space=pltpu.VMEM)
    send_dev, send_lev, own = pl.pallas_call(
        terms_kernel,
        name="terms",
        in_specs=[anywhere] * 11,
        out_specs=[vmem] * 3,
        out_shape=[
            pltpu.VMEM((peers, ROWS, CELLS), BF16),
            pltpu.VMEM((levels, ROWS, CELLS), BF16),
            pltpu.VMEM((rows, CELLS), F32),
        ],
        scratch_shapes=[
            pltpu.VMEM((rows, CELLS), F32),
            pltpu.VMEM((BLK + 1, ROWS, CELLS), F32),
            pltpu.VMEM((BLK + 1, ROWS, CELLS), F32),
            pltpu.VMEM((BLK + 1, ROWS, CELLS), BF16),
            pltpu.VMEM((BLK + 1, ROWS, CELLS), BF16),
            pltpu.VMEM((peers, CAP * CELLS, CELLS), BF16),
            pltpu.VMEM((levels, CAP * CELLS, CELLS), BF16),
            pltpu.VMEM((BLK, CELLS, CELLS), BF16),
            pltpu.SMEM((1, BLK), jnp.int32),
            pltpu.SMEM((CAP, peers), jnp.int32),
            pltpu.SMEM((CAP, peers), jnp.int32),
            pltpu.SMEM((1, peers), jnp.int32),
            pltpu.SMEM((CAP, levels), jnp.int32),
            pltpu.SMEM((CAP, levels), jnp.int32),
            pltpu.SMEM((1, levels), jnp.int32),
            pltpu.SemaphoreType.DMA((8,)),
            pltpu.SemaphoreType.DMA((W_CHUNKS + 2,)),
        ],
    )(
        flat,
        own_src,
        own_weight[0],
        send_block[0, 0].T,
        send_target[0, 0].T,
        send_count[0],
        send_weight.reshape(peers, CAP * CELLS, CELLS),
        left_block[0, 0].T,
        left_target[0, 0].T,
        left_count[0],
        left_weight.reshape(levels, CAP * CELLS, CELLS),
    )
    sends = {"dev": send_dev, "level": send_lev}
    early = exchange(sends[ORDER[0]], ORDER[0])
    second = sends[ORDER[1]]
    second = pl.pallas_call(
        relay_kernel,
        name="relay",
        in_specs=[vmem, vmem],
        out_specs=vmem,
        out_shape=pltpu.VMEM(second.shape, BF16),
        input_output_aliases={1: 0},
    )(early, in_vmem(second))
    late = exchange(second, ORDER[1])
    remapped, totals = pl.pallas_call(
        final_kernel,
        name="final",
        in_specs=[vmem, vmem, vmem],
        out_specs=[vmem, vmem],
        out_shape=[
            jax.ShapeDtypeStruct((rows, CELLS), F32),
            jax.ShapeDtypeStruct((1, COMP), F32),
        ],
    )(early, late, in_vmem(own))
    remapped = jnp.transpose(remapped.reshape(COMP, BLK, CELLS), (1, 0, 2))
    return (remapped[None], totals.reshape(COMP))


def solution(mesh):
    return jax.shard_map(
        body,
        mesh=mesh,
        in_specs=(
            P("level", "dev", None, None),
            P("level", "dev"),
            P("level", "dev", None, None),
            P("level", "dev", None, None),
            P("level", "dev", None, None),
            P("level", "dev", None),
            P("level", "dev", None, None, None, None),
            P("level", "dev", None, None),
            P("level", "dev", None, None),
            P("level", "dev", None),
            P("level", "dev", None, None, None, None),
        ),
        out_specs=(P("level", "dev", None, None), P()),
        check_vma=False,
    )
```

```python
import jax
import jax.numpy as jnp
from jax import lax
from jax.experimental import pallas as pl
from jax.experimental.pallas import tpu as pltpu
from jax.sharding import PartitionSpec as P

GROUPS = {
    "dev": [21, 22, 23, 24, 25, 26, 27, 28, 29, 30, 31, 0, 1, 2, 3, 4, 5, 6, 7, 8, 9, 10, 11, 12, 13, 14, 15, 16, 17, 18, 19, 20],
    "level": [10, 0, 1, 2, 3, 15, 4, 14, 5, 13, 6, 12, 7, 11, 8, 9],
}
ORDER = ("dev", "level")
COMP = 12
CELLS = 128
BLK = 16
CAP = 2
ROWS = 26
PAIRS = ROWS // 2
GROUP = 4
PART = 32
W_CHUNKS = 4
F32 = jnp.float32
BF16 = jnp.bfloat16


def code_tile(t0, t1, slot):
    row = lax.broadcasted_iota(jnp.int32, (8, CELLS), 0)
    r = lax.broadcasted_iota(jnp.int32, (8, CELLS), 1) - slot * ROWS
    here = (row == 0) & (r >= 0) & (r < ROWS)
    second = r >= COMP
    comp = jnp.where(second, r - COMP, r)
    code = comp * BLK + jnp.where(second, t1, t0)
    code = jnp.where(r < CAP * COMP, code, 255)
    return jnp.where(here, code, 0).astype(F32)


def three_parts(total):
    row = lax.broadcasted_iota(jnp.int32, (8, CELLS), 0)
    full = jnp.broadcast_to(total, (8, CELLS))
    hi = full.astype(BF16).astype(F32)
    mid = (full - hi).astype(BF16).astype(F32)
    low = full - hi - mid
    parts = hi + pltpu.roll(mid, PART, 1) + pltpu.roll(low, 2 * PART, 1)
    return jnp.where(row == 1, parts, jnp.zeros_like(parts))


def sum_parts(row):
    full = jnp.broadcast_to(row, (8, CELLS))
    full = full + pltpu.roll(full, CELLS - PART, 1) + pltpu.roll(full, CELLS - 2 * PART, 1)
    lane = lax.broadcasted_iota(jnp.int32, (8, CELLS), 1)
    return jnp.where(lane < CAP * COMP, full, jnp.zeros_like(full))


def last_pair(recv, sl):
    return jnp.sum(recv[sl, PAIRS - 1].astype(F32), axis=0)


def terms_kernel(
    fields,
    own_src,
    own_w,
    send_blk,
    send_tgt,
    send_cnt,
    send_w,
    left_blk,
    left_tgt,
    left_cnt,
    left_w,
    out_dev,
    out_lev,
    own_out,
    fld,
    first32,
    second32,
    first,
    second,
    wd,
    wl,
    wo,
    s_src,
    s_sblk,
    s_stgt,
    s_scnt,
    s_lblk,
    s_ltgt,
    s_lcnt,
    sems,
    wsems,
):
    peers = send_w.shape[0]
    levels = left_w.shape[0]
    small = []
    pairs = (
        (fields, fld),
        (own_src, s_src),
        (send_blk, s_sblk),
        (send_tgt, s_stgt),
        (send_cnt, s_scnt),
        (left_blk, s_lblk),
        (left_tgt, s_ltgt),
        (left_cnt, s_lcnt),
    )
    copy = pltpu.make_async_copy(fields, fld, sems.at[0])
    copy.start()
    small.append(copy)
    step = peers // W_CHUNKS
    weights = []
    for n in range(W_CHUNKS):
        sl = pl.ds(n * step, step)
        copy = pltpu.make_async_copy(send_w.at[sl], wd.at[sl], wsems.at[n])
        copy.start()
        weights.append(copy)
    left_copy = pltpu.make_async_copy(left_w, wl, wsems.at[W_CHUNKS])
    left_copy.start()
    own_copy = pltpu.make_async_copy(own_w, wo, wsems.at[W_CHUNKS + 1])
    own_copy.start()

    for n, (src, dst) in enumerate(pairs[1:], 1):
        copy = pltpu.make_async_copy(src, dst, sems.at[n])
        copy.start()
        small.append(copy)
    first32[...] = jnp.zeros(first32.shape, F32)
    second32[...] = jnp.zeros(second32.shape, F32)
    small[0].wait()
    for b in range(BLK):
        one = fld[pl.ds(b, COMP, stride=BLK), :]
        first32[b, 0:COMP, :] = one
        second32[b, COMP : 2 * COMP, :] = one
    first[...] = first32[...].astype(BF16)
    second[...] = second32[...].astype(BF16)
    for copy in small[1:]:
        copy.wait()

    def group_terms(out, blk, tgt, cnt, weight, axis):
        size = out.shape[0]
        here = lax.axis_index(axis)
        slot = jnp.int32(0)
        for n, member in enumerate(GROUPS[axis]):
            slot = jnp.where(here == member, n % GROUP, slot)

        def one(n, acc):
            live = cnt[0, n]
            b0 = jnp.where(live > 0, blk[0, n], BLK)
            b1 = jnp.where(live > 1, blk[1, n], BLK)
            lhs = jnp.concatenate([first[b0], second[b1]], axis=1)
            t = jnp.dot(lhs, weight[n], preferred_element_type=F32)
            to = GROUPS[axis].index(n)
            flat = out.reshape(size * ROWS, CELLS)
            codes = code_tile(tgt[0, n], tgt[1, n], slot)
            message = jnp.concatenate([t[0:24], codes], axis=0).astype(BF16)
            flat[to * ROWS : (to + 1) * ROWS, :] = message[0:ROWS]
            return acc + t[0:24]

        return one

    dev_step = group_terms(out_dev, s_sblk, s_stgt, s_scnt, wd, "dev")
    lev_step = group_terms(out_lev, s_lblk, s_ltgt, s_lcnt, wl, "level")
    acc = jnp.zeros((24, CELLS), F32)
    for n in range(W_CHUNKS):
        weights[n].wait()
        for peer in range(n * step, (n + 1) * step):
            acc = dev_step(peer, acc)
    left_copy.wait()
    for level in range(levels):
        acc = lev_step(level, acc)
    own_copy.wait()
    own_acc = jnp.zeros((16, CELLS), F32)
    for b in range(BLK):
        t = jnp.dot(first[s_src[0, b], 0:16, :], wo[b], preferred_element_type=F32)
        own_out[pl.ds(b, COMP, stride=BLK), :] = t[0:COMP]
        own_acc = own_acc + t
    own_acc = jnp.concatenate([own_acc, jnp.zeros((8, CELLS), F32)], axis=0)
    acc = jnp.concatenate([acc + own_acc, jnp.zeros((CELLS - 24, CELLS), F32)], axis=0)
    sums = lax.dot_general(
        jnp.ones((8, CELLS), F32),
        acc,
        (((1,), (1,)), ((), ())),
        precision=lax.Precision.HIGHEST,
        preferred_element_type=F32,
    )
    add_parts(out_dev if ORDER[0] == "dev" else out_lev, sums[0:1])


def add_parts(message, total):
    pair = message[:, PAIRS - 1].astype(F32) + three_parts(total)[0:2][None]
    message[:, PAIRS - 1] = pair.astype(BF16)


def relay_kernel(recv, send_in, send_out):
    del send_in
    add_parts(send_out, sum_parts(last_pair(recv, slice(None))[1:2])[0:1])


def placed(recv):
    peers = recv.shape[0]
    flat = recv.reshape(peers * ROWS, CELLS)
    row = lax.broadcasted_iota(jnp.int32, (COMP * BLK, CELLS), 0).astype(F32)
    total = jnp.zeros((COMP * BLK, CELLS), F32)
    for g in range(peers // GROUP):
        codes = last_pair(recv, slice(g * GROUP, (g + 1) * GROUP))[0:1]
        pick = jnp.where(row == codes, 1.0, 0.0).astype(BF16)[:, : GROUP * ROWS]
        data = flat[g * GROUP * ROWS : (g + 1) * GROUP * ROWS, :]
        total = total + jnp.dot(pick, data, preferred_element_type=F32)
    return total


def final_kernel(early, late, own, out, totals):
    out[...] = own[...] + placed(early) + placed(late)
    both = sum_parts(last_pair(late, slice(None))[1:2])
    both = both + pltpu.roll(both, CELLS - COMP, 1)
    totals[...] = both[0:1, 0:COMP] * (1.0 / (CELLS * BLK))


def in_vmem(x):
    return pltpu.with_memory_space_constraint(x, pltpu.VMEM)


def exchange(message, axis):
    groups = [GROUPS[axis]]
    got = lax.all_to_all(in_vmem(message), axis, 0, 0, axis_index_groups=groups, tiled=True)
    return in_vmem(got)


def body(
    fields,
    own_src,
    own_weight,
    send_block,
    send_target,
    send_count,
    send_weight,
    left_block,
    left_target,
    left_count,
    left_weight,
):
    peers = send_weight.shape[2]
    levels = left_weight.shape[2]
    rows = COMP * BLK
    flat = jnp.transpose(fields[0], (1, 0, 2)).reshape(rows, CELLS)
    anywhere = pl.BlockSpec(memory_space=pl.ANY)
    vmem = pl.BlockSpec(memory_space=pltpu.VMEM)
    send_dev, send_lev, own = pl.pallas_call(
        terms_kernel,
        name="terms",
        in_specs=[anywhere] * 11,
        out_specs=[vmem] * 3,
        out_shape=[
            pltpu.VMEM((peers, PAIRS, 2, CELLS), BF16),
            pltpu.VMEM((levels, PAIRS, 2, CELLS), BF16),
            pltpu.VMEM((rows, CELLS), F32),
        ],
        scratch_shapes=[
            pltpu.VMEM((rows, CELLS), F32),
            pltpu.VMEM((BLK + 1, 32, CELLS), F32),
            pltpu.VMEM((BLK + 1, 32, CELLS), F32),
            pltpu.VMEM((BLK + 1, 32, CELLS), BF16),
            pltpu.VMEM((BLK + 1, 32, CELLS), BF16),
            pltpu.VMEM((peers, CAP * CELLS, CELLS), BF16),
            pltpu.VMEM((levels, CAP * CELLS, CELLS), BF16),
            pltpu.VMEM((BLK, CELLS, CELLS), BF16),
            pltpu.SMEM((1, BLK), jnp.int32),
            pltpu.SMEM((CAP, peers), jnp.int32),
            pltpu.SMEM((CAP, peers), jnp.int32),
            pltpu.SMEM((1, peers), jnp.int32),
            pltpu.SMEM((CAP, levels), jnp.int32),
            pltpu.SMEM((CAP, levels), jnp.int32),
            pltpu.SMEM((1, levels), jnp.int32),
            pltpu.SemaphoreType.DMA((8,)),
            pltpu.SemaphoreType.DMA((W_CHUNKS + 2,)),
        ],
    )(
        flat,
        own_src,
        own_weight[0],
        send_block[0, 0].T,
        send_target[0, 0].T,
        send_count[0],
        send_weight.reshape(peers, CAP * CELLS, CELLS),
        left_block[0, 0].T,
        left_target[0, 0].T,
        left_count[0],
        left_weight.reshape(levels, CAP * CELLS, CELLS),
    )
    sends = {"dev": send_dev, "level": send_lev}
    early = exchange(sends[ORDER[0]], ORDER[0])
    second = sends[ORDER[1]]
    second = pl.pallas_call(
        relay_kernel,
        name="relay",
        in_specs=[vmem, vmem],
        out_specs=vmem,
        out_shape=pltpu.VMEM(second.shape, BF16),
        input_output_aliases={1: 0},
    )(early, in_vmem(second))
    late = exchange(second, ORDER[1])
    remapped, totals = pl.pallas_call(
        final_kernel,
        name="final",
        in_specs=[vmem, vmem, vmem],
        out_specs=[vmem, vmem],
        out_shape=[
            jax.ShapeDtypeStruct((rows, CELLS), F32),
            jax.ShapeDtypeStruct((1, COMP), F32),
        ],
    )(early, late, in_vmem(own))
    remapped = jnp.transpose(remapped.reshape(COMP, BLK, CELLS), (1, 0, 2))
    return (remapped[None], totals.reshape(COMP))


def solution(mesh):
    return jax.shard_map(
        body,
        mesh=mesh,
        in_specs=(
            P("level", "dev", None, None),
            P("level", "dev"),
            P("level", "dev", None, None),
            P("level", "dev", None, None),
            P("level", "dev", None, None),
            P("level", "dev", None),
            P("level", "dev", None, None, None, None),
            P("level", "dev", None, None),
            P("level", "dev", None, None),
            P("level", "dev", None),
            P("level", "dev", None, None, None, None),
        ),
        out_specs=(P("level", "dev", None, None), P()),
        check_vma=False,
    )
```

```python
import functools

import jax
import jax.numpy as jnp
from jax import lax
from jax.experimental import pallas as pl
from jax.experimental.pallas import tpu as pltpu
from jax.sharding import PartitionSpec as P

GROUPS = {
    "dev": [21, 22, 23, 24, 25, 26, 27, 28, 29, 30, 31, 0, 1, 2, 3, 4, 5, 6, 7, 8, 9, 10, 11, 12, 13, 14, 15, 16, 17, 18, 19, 20],
    "level": [10, 0, 1, 2, 3, 15, 4, 14, 5, 13, 6, 12, 7, 11, 8, 9],
}
ORDER = ("dev", "level")
WAITING = 8
COMP = 12
CELLS = 128
BLK = 16
CAP = 2
ROWS = 26
PAIRS = ROWS // 2
GROUP = 4
PART = 32
W_CHUNKS = 2
F32 = jnp.float32
BF16 = jnp.bfloat16


def code_tile(t0, t1, slot):
    row = lax.broadcasted_iota(jnp.int32, (8, CELLS), 0)
    r = lax.broadcasted_iota(jnp.int32, (8, CELLS), 1) - slot * ROWS
    here = (row == 0) & (r >= 0) & (r < ROWS)
    second = r >= COMP
    comp = jnp.where(second, r - COMP, r)
    code = comp * BLK + jnp.where(second, t1, t0)
    code = jnp.where(r < CAP * COMP, code, 255)
    return jnp.where(here, code, 0).astype(F32)


def three_parts(total):
    row = lax.broadcasted_iota(jnp.int32, (8, CELLS), 0)
    full = jnp.broadcast_to(total, (8, CELLS))
    hi = full.astype(BF16).astype(F32)
    mid = (full - hi).astype(BF16).astype(F32)
    low = full - hi - mid
    parts = hi + pltpu.roll(mid, PART, 1) + pltpu.roll(low, 2 * PART, 1)
    return jnp.where(row == 1, parts, jnp.zeros_like(parts))


def sum_parts(row):
    full = jnp.broadcast_to(row, (8, CELLS))
    full = full + pltpu.roll(full, CELLS - PART, 1) + pltpu.roll(full, CELLS - 2 * PART, 1)
    lane = lax.broadcasted_iota(jnp.int32, (8, CELLS), 1)
    return jnp.where(lane < CAP * COMP, full, jnp.zeros_like(full))


def last_pair(recv, sl):
    return jnp.sum(recv[sl, PAIRS - 1].astype(F32), axis=0)


def terms_kernel(
    fields,
    own_src,
    own_w,
    send_blk,
    send_tgt,
    send_cnt,
    send_w,
    left_blk,
    left_tgt,
    left_cnt,
    left_w,
    out_dev,
    out_lev,
    own_out,
    fld,
    first32,
    second32,
    first,
    second,
    wd,
    wl,
    wo,
    s_src,
    s_sblk,
    s_stgt,
    s_scnt,
    s_lblk,
    s_ltgt,
    s_lcnt,
    sems,
    wsems,
):
    peers = send_w.shape[0]
    levels = left_w.shape[0]
    small = []
    pairs = (
        (fields, fld),
        (own_src, s_src),
        (send_blk, s_sblk),
        (send_tgt, s_stgt),
        (send_cnt, s_scnt),
        (left_blk, s_lblk),
        (left_tgt, s_ltgt),
        (left_cnt, s_lcnt),
    )
    copy = pltpu.make_async_copy(fields, fld, sems.at[0])
    copy.start()
    small.append(copy)
    step = peers // W_CHUNKS
    left_copy = pltpu.make_async_copy(left_w, wl, wsems.at[W_CHUNKS])
    left_copy.start()
    own_copy = pltpu.make_async_copy(own_w, wo, wsems.at[W_CHUNKS + 1])
    own_copy.start()
    weights = []
    for n in range(W_CHUNKS):
        sl = pl.ds(n * step, step)
        copy = pltpu.make_async_copy(send_w.at[sl], wd.at[sl], wsems.at[n])
        copy.start()
        weights.append(copy)

    for n, (src, dst) in enumerate(pairs[1:], 1):
        copy = pltpu.make_async_copy(src, dst, sems.at[n])
        copy.start()
        small.append(copy)
    first32[...] = jnp.zeros(first32.shape, F32)
    second32[...] = jnp.zeros(second32.shape, F32)
    small[0].wait()
    for b in range(BLK):
        one = fld[pl.ds(b, COMP, stride=BLK), :]
        first32[b, 0:COMP, :] = one
        second32[b, COMP : 2 * COMP, :] = one
    first[...] = first32[...].astype(BF16)
    second[...] = second32[...].astype(BF16)
    for copy in small[1:]:
        copy.wait()

    def group_terms(out, blk, tgt, cnt, weight, axis):
        size = out.shape[0]
        here = lax.axis_index(axis)
        slot = jnp.int32(0)
        for n, member in enumerate(GROUPS[axis]):
            slot = jnp.where(here == member, n % GROUP, slot)

        def one(n, acc):
            live = cnt[0, n]
            b0 = jnp.where(live > 0, blk[0, n], BLK)
            b1 = jnp.where(live > 1, blk[1, n], BLK)
            lhs = jnp.concatenate([first[b0], second[b1]], axis=1)
            t = jnp.dot(lhs, weight[n], preferred_element_type=F32)
            to = GROUPS[axis].index(n)
            flat = out.reshape(size * ROWS, CELLS)
            codes = code_tile(tgt[0, n], tgt[1, n], slot)
            message = jnp.concatenate([t[0:24], codes], axis=0).astype(BF16)
            flat[to * ROWS : (to + 1) * ROWS, :] = message[0:ROWS]
            return acc + t[0:24]

        return one

    dev_step = group_terms(out_dev, s_sblk, s_stgt, s_scnt, wd, "dev")
    lev_step = group_terms(out_lev, s_lblk, s_ltgt, s_lcnt, wl, "level")
    acc = jnp.zeros((24, CELLS), F32)
    left_copy.wait()
    own_copy.wait()
    for level in range(levels):
        acc = lev_step(level, acc)
    own_acc = jnp.zeros((16, CELLS), F32)
    for b in range(BLK):
        t = jnp.dot(first[s_src[0, b], 0:16, :], wo[b], preferred_element_type=F32)
        own_out[pl.ds(b, COMP, stride=BLK), :] = t[0:COMP]
        own_acc = own_acc + t
    for n in range(W_CHUNKS):
        weights[n].wait()
        for peer in range(n * step, (n + 1) * step):
            acc = dev_step(peer, acc)
    own_acc = jnp.concatenate([own_acc, jnp.zeros((8, CELLS), F32)], axis=0)
    acc = jnp.concatenate([acc + own_acc, jnp.zeros((CELLS - 24, CELLS), F32)], axis=0)
    sums = lax.dot_general(
        jnp.ones((8, CELLS), F32),
        acc,
        (((1,), (1,)), ((), ())),
        precision=lax.Precision.HIGHEST,
        preferred_element_type=F32,
    )
    add_parts(out_dev if ORDER[0] == "dev" else out_lev, sums[0:1])


def scoped_terms(*refs):
    pl.run_scoped(
        functools.partial(terms_kernel, *refs),
        pltpu.SemaphoreType.DMA((8,)),
        pltpu.SemaphoreType.DMA((W_CHUNKS + 2,)),
    )


def add_parts(message, total):
    pair = message[:, PAIRS - 1].astype(F32) + three_parts(total)[0:2][None]
    message[:, PAIRS - 1] = pair.astype(BF16)


def places_early():
    return lax.axis_index("level") < WAITING


def relay_kernel(recv, own, send_in, send_out, base):
    del send_in
    add_parts(send_out, sum_parts(last_pair(recv, slice(None))[1:2])[0:1])

    @pl.when(places_early())
    def _():
        base[...] = own[...] + placed(recv)

    @pl.when(jnp.logical_not(places_early()))
    def _():
        base[...] = own[...]


def placed(recv):
    peers = recv.shape[0]
    flat = recv.reshape(peers * ROWS, CELLS)
    row = lax.broadcasted_iota(jnp.int32, (COMP * BLK, CELLS), 0).astype(F32)
    total = jnp.zeros((COMP * BLK, CELLS), F32)
    for g in range(peers // GROUP):
        codes = last_pair(recv, slice(g * GROUP, (g + 1) * GROUP))[0:1]
        pick = jnp.where(row == codes, 1.0, 0.0).astype(BF16)[:, : GROUP * ROWS]
        data = flat[g * GROUP * ROWS : (g + 1) * GROUP * ROWS, :]
        total = total + jnp.dot(pick, data, preferred_element_type=F32)
    return total


def final_kernel(early, late, base, out, totals):
    out[...] = base[...] + placed(late)

    @pl.when(jnp.logical_not(places_early()))
    def _():
        out[...] += placed(early)

    both = sum_parts(last_pair(late, slice(None))[1:2])
    both = both + pltpu.roll(both, CELLS - COMP, 1)
    totals[...] = both[0:1, 0:COMP] * (1.0 / (CELLS * BLK))


def in_vmem(x):
    return pltpu.with_memory_space_constraint(x, pltpu.VMEM)


def exchange(message, axis):
    groups = [GROUPS[axis]]
    got = lax.all_to_all(in_vmem(message), axis, 0, 0, axis_index_groups=groups, tiled=True)
    return in_vmem(got)


def body(
    fields,
    own_src,
    own_weight,
    send_block,
    send_target,
    send_count,
    send_weight,
    left_block,
    left_target,
    left_count,
    left_weight,
):
    peers = send_weight.shape[2]
    levels = left_weight.shape[2]
    rows = COMP * BLK
    flat = jnp.transpose(fields[0], (1, 0, 2)).reshape(rows, CELLS)
    anywhere = pl.BlockSpec(memory_space=pl.ANY)
    vmem = pl.BlockSpec(memory_space=pltpu.VMEM)
    send_dev, send_lev, own = pl.pallas_call(
        scoped_terms,
        name="terms",
        in_specs=[anywhere] * 11,
        out_specs=[vmem] * 3,
        out_shape=[
            pltpu.VMEM((peers, PAIRS, 2, CELLS), BF16),
            pltpu.VMEM((levels, PAIRS, 2, CELLS), BF16),
            pltpu.VMEM((rows, CELLS), F32),
        ],
        scratch_shapes=[
            pltpu.VMEM((rows, CELLS), F32),
            pltpu.VMEM((BLK + 1, 32, CELLS), F32),
            pltpu.VMEM((BLK + 1, 32, CELLS), F32),
            pltpu.VMEM((BLK + 1, 32, CELLS), BF16),
            pltpu.VMEM((BLK + 1, 32, CELLS), BF16),
            pltpu.VMEM((peers, CAP * CELLS, CELLS), BF16),
            pltpu.VMEM((levels, CAP * CELLS, CELLS), BF16),
            pltpu.VMEM((BLK, CELLS, CELLS), BF16),
            pltpu.SMEM((1, BLK), jnp.int32),
            pltpu.SMEM((CAP, peers), jnp.int32),
            pltpu.SMEM((CAP, peers), jnp.int32),
            pltpu.SMEM((1, peers), jnp.int32),
            pltpu.SMEM((CAP, levels), jnp.int32),
            pltpu.SMEM((CAP, levels), jnp.int32),
            pltpu.SMEM((1, levels), jnp.int32),
        ],
    )(
        flat,
        own_src,
        own_weight[0],
        send_block[0, 0].T,
        send_target[0, 0].T,
        send_count[0],
        send_weight.reshape(peers, CAP * CELLS, CELLS),
        left_block[0, 0].T,
        left_target[0, 0].T,
        left_count[0],
        left_weight.reshape(levels, CAP * CELLS, CELLS),
    )
    sends = {"dev": send_dev, "level": send_lev}
    early = exchange(sends[ORDER[0]], ORDER[0])
    second = sends[ORDER[1]]
    second, base = pl.pallas_call(
        relay_kernel,
        name="relay",
        in_specs=[vmem] * 3,
        out_specs=[vmem] * 2,
        out_shape=[pltpu.VMEM(second.shape, BF16), pltpu.VMEM((rows, CELLS), F32)],
        input_output_aliases={2: 0},
    )(early, in_vmem(own), in_vmem(second))
    late = exchange(second, ORDER[1])
    remapped, totals = pl.pallas_call(
        final_kernel,
        name="final",
        in_specs=[vmem, vmem, vmem],
        out_specs=[vmem, vmem],
        out_shape=[
            jax.ShapeDtypeStruct((rows, CELLS), F32),
            jax.ShapeDtypeStruct((1, COMP), F32),
        ],
    )(early, late, in_vmem(base))
    remapped = jnp.transpose(remapped.reshape(COMP, BLK, CELLS), (1, 0, 2))
    return (remapped[None], totals.reshape(COMP))


def solution(mesh):
    return jax.shard_map(
        body,
        mesh=mesh,
        in_specs=(
            P("level", "dev", None, None),
            P("level", "dev"),
            P("level", "dev", None, None),
            P("level", "dev", None, None),
            P("level", "dev", None, None),
            P("level", "dev", None),
            P("level", "dev", None, None, None, None),
            P("level", "dev", None, None),
            P("level", "dev", None, None),
            P("level", "dev", None),
            P("level", "dev", None, None, None, None),
        ),
        out_specs=(P("level", "dev", None, None), P()),
        check_vma=False,
    )
```

```python
import functools

import jax
import jax.numpy as jnp
from jax import lax
from jax.experimental import pallas as pl
from jax.experimental.pallas import tpu as pltpu
from jax.sharding import PartitionSpec as P

GROUPS = {
    "dev": [21, 22, 23, 24, 25, 26, 27, 28, 29, 30, 31, 0, 1, 2, 3, 4, 5, 6, 7, 8, 9, 10, 11, 12, 13, 14, 15, 16, 17, 18, 19, 20],
    "level": [10, 0, 1, 2, 3, 15, 4, 14, 5, 13, 6, 12, 7, 11, 8, 9],
}
ORDER = ("dev", "level")
WAITING = 8
COMP = 12
CELLS = 128
BLK = 16
CAP = 2
ROWS = 26
PAIRS = ROWS // 2
GROUP = 4
PART = 32
W_CHUNKS = 2
F32 = jnp.float32
BF16 = jnp.bfloat16


def code_tile(t0, t1, slot):
    row = lax.broadcasted_iota(jnp.int32, (8, CELLS), 0)
    r = lax.broadcasted_iota(jnp.int32, (8, CELLS), 1) - slot * ROWS
    here = (row == 0) & (r >= 0) & (r < ROWS)
    second = r >= COMP
    comp = jnp.where(second, r - COMP, r)
    code = comp * BLK + jnp.where(second, t1, t0)
    code = jnp.where(r < CAP * COMP, code, 255)
    return jnp.where(here, code, 0).astype(F32)


def three_parts(total):
    row = lax.broadcasted_iota(jnp.int32, (8, CELLS), 0)
    full = jnp.broadcast_to(total, (8, CELLS))
    hi = full.astype(BF16).astype(F32)
    mid = (full - hi).astype(BF16).astype(F32)
    low = full - hi - mid
    parts = hi + pltpu.roll(mid, PART, 1) + pltpu.roll(low, 2 * PART, 1)
    return jnp.where(row == 1, parts, jnp.zeros_like(parts))


def sum_parts(row):
    full = jnp.broadcast_to(row, (8, CELLS))
    full = full + pltpu.roll(full, CELLS - PART, 1) + pltpu.roll(full, CELLS - 2 * PART, 1)
    lane = lax.broadcasted_iota(jnp.int32, (8, CELLS), 1)
    return jnp.where(lane < CAP * COMP, full, jnp.zeros_like(full))


def last_pair(recv, sl):
    return jnp.sum(recv[sl, PAIRS - 1].astype(F32), axis=0)


def terms_kernel(
    fields,
    own_src,
    own_w,
    send_blk,
    send_tgt,
    send_cnt,
    send_w,
    left_blk,
    left_tgt,
    left_cnt,
    left_w,
    out_dev,
    out_lev,
    own_out,
    fld,
    first32,
    second32,
    first,
    second,
    wd,
    wl,
    wo,
    s_src,
    s_sblk,
    s_stgt,
    s_scnt,
    s_lblk,
    s_ltgt,
    s_lcnt,
    sems,
    wsems,
):
    peers = send_w.shape[0]
    levels = left_w.shape[0]
    small = []
    pairs = (
        (fields, fld),
        (own_src, s_src),
        (send_blk, s_sblk),
        (send_tgt, s_stgt),
        (send_cnt, s_scnt),
        (left_blk, s_lblk),
        (left_tgt, s_ltgt),
        (left_cnt, s_lcnt),
    )
    copy = pltpu.make_async_copy(fields, fld, sems.at[0])
    copy.start()
    small.append(copy)
    step = peers // W_CHUNKS
    left_copy = pltpu.make_async_copy(left_w, wl, wsems.at[W_CHUNKS])
    left_copy.start()
    own_copy = pltpu.make_async_copy(own_w, wo, wsems.at[W_CHUNKS + 1])
    own_copy.start()
    weights = []
    for n in range(W_CHUNKS):
        sl = pl.ds(n * step, step)
        copy = pltpu.make_async_copy(send_w.at[sl], wd.at[sl], wsems.at[n])
        copy.start()
        weights.append(copy)

    for n, (src, dst) in enumerate(pairs[1:], 1):
        copy = pltpu.make_async_copy(src, dst, sems.at[n])
        copy.start()
        small.append(copy)
    first32[...] = jnp.zeros(first32.shape, F32)
    second32[...] = jnp.zeros(second32.shape, F32)
    small[0].wait()
    for b in range(BLK):
        one = fld[pl.ds(b, COMP, stride=BLK), :]
        first32[b, 0:COMP, :] = one
        second32[b, COMP : 2 * COMP, :] = one
    first[...] = first32[...].astype(BF16)
    second[...] = second32[...].astype(BF16)
    for copy in small[1:]:
        copy.wait()

    def group_terms(out, blk, tgt, cnt, weight, axis):
        size = out.shape[0]
        here = lax.axis_index(axis)
        slot = jnp.int32(0)
        for n, member in enumerate(GROUPS[axis]):
            slot = jnp.where(here == member, n % GROUP, slot)

        def one(n, acc):
            live = cnt[0, n]
            b0 = jnp.where(live > 0, blk[0, n], BLK)
            b1 = jnp.where(live > 1, blk[1, n], BLK)
            lhs = jnp.concatenate([first[b0], second[b1]], axis=1)
            t = jnp.dot(lhs, weight[n], preferred_element_type=F32)
            to = GROUPS[axis].index(n)
            flat = out.reshape(size * ROWS, CELLS)
            codes = code_tile(tgt[0, n], tgt[1, n], slot)
            message = jnp.concatenate([t[0:24], codes], axis=0).astype(BF16)
            flat[to * ROWS : (to + 1) * ROWS, :] = message[0:ROWS]
            return acc + t[0:24]

        return one

    dev_step = group_terms(out_dev, s_sblk, s_stgt, s_scnt, wd, "dev")
    lev_step = group_terms(out_lev, s_lblk, s_ltgt, s_lcnt, wl, "level")
    acc = jnp.zeros((24, CELLS), F32)
    left_copy.wait()
    own_copy.wait()
    for level in range(levels):
        acc = lev_step(level, acc)
    own_acc = jnp.zeros((16, CELLS), F32)
    for b in range(BLK):
        t = jnp.dot(first[s_src[0, b], 0:16, :], wo[b], preferred_element_type=F32)
        own_out[pl.ds(b, COMP, stride=BLK), :] = t[0:COMP]
        own_acc = own_acc + t
    for n in range(W_CHUNKS):
        weights[n].wait()
        for peer in range(n * step, (n + 1) * step):
            acc = dev_step(peer, acc)
    acc = acc + jnp.concatenate([own_acc, jnp.zeros((8, CELLS), F32)], axis=0)
    row = lax.broadcasted_iota(jnp.int32, acc.shape, 0)
    lane = lax.broadcasted_iota(jnp.int32, acc.shape, 1)
    sums = jnp.where(row == lane, jnp.sum(acc, axis=1, keepdims=True), jnp.zeros_like(acc))
    sums = jnp.sum(sums, axis=0, keepdims=True)
    add_parts(out_dev if ORDER[0] == "dev" else out_lev, sums[0:1])


def scoped_terms(*refs):
    pl.run_scoped(
        functools.partial(terms_kernel, *refs),
        pltpu.SemaphoreType.DMA((8,)),
        pltpu.SemaphoreType.DMA((W_CHUNKS + 2,)),
    )


def add_parts(message, total):
    pair = message[:, PAIRS - 1].astype(F32) + three_parts(total)[0:2][None]
    message[:, PAIRS - 1] = pair.astype(BF16)


def places_early():
    return lax.axis_index("level") < WAITING


def relay_kernel(recv, own, send_in, send_out, base):
    del send_in
    add_parts(send_out, sum_parts(last_pair(recv, slice(None))[1:2])[0:1])

    @pl.when(places_early())
    def _():
        base[...] = own[...] + placed(recv)

    @pl.when(jnp.logical_not(places_early()))
    def _():
        base[...] = own[...]


def placed(recv):
    peers = recv.shape[0]
    flat = recv.reshape(peers * ROWS, CELLS)
    row = lax.broadcasted_iota(jnp.int32, (COMP * BLK, CELLS), 0).astype(F32)
    total = jnp.zeros((COMP * BLK, CELLS), F32)
    for g in range(peers // GROUP):
        codes = last_pair(recv, slice(g * GROUP, (g + 1) * GROUP))[0:1]
        pick = jnp.where(row == codes, 1.0, 0.0).astype(BF16)[:, : GROUP * ROWS]
        data = flat[g * GROUP * ROWS : (g + 1) * GROUP * ROWS, :]
        total = total + jnp.dot(pick, data, preferred_element_type=F32)
    return total


def final_kernel(early, late, base, out, totals):
    out[...] = base[...] + placed(late)

    @pl.when(jnp.logical_not(places_early()))
    def _():
        out[...] += placed(early)

    both = sum_parts(last_pair(late, slice(None))[1:2])
    both = both + pltpu.roll(both, CELLS - COMP, 1)
    totals[...] = both[0:1, 0:COMP] * (1.0 / (CELLS * BLK))


def in_vmem(x):
    return pltpu.with_memory_space_constraint(x, pltpu.VMEM)


def exchange(message, axis):
    groups = [GROUPS[axis]]
    got = lax.all_to_all(in_vmem(message), axis, 0, 0, axis_index_groups=groups, tiled=True)
    return in_vmem(got)


def body(
    fields,
    own_src,
    own_weight,
    send_block,
    send_target,
    send_count,
    send_weight,
    left_block,
    left_target,
    left_count,
    left_weight,
):
    peers = send_weight.shape[2]
    levels = left_weight.shape[2]
    rows = COMP * BLK
    flat = jnp.transpose(fields[0], (1, 0, 2)).reshape(rows, CELLS)
    anywhere = pl.BlockSpec(memory_space=pl.ANY)
    vmem = pl.BlockSpec(memory_space=pltpu.VMEM)
    send_dev, send_lev, own = pl.pallas_call(
        scoped_terms,
        name="terms",
        in_specs=[anywhere] * 11,
        out_specs=[vmem] * 3,
        out_shape=[
            pltpu.VMEM((peers, PAIRS, 2, CELLS), BF16),
            pltpu.VMEM((levels, PAIRS, 2, CELLS), BF16),
            pltpu.VMEM((rows, CELLS), F32),
        ],
        scratch_shapes=[
            pltpu.VMEM((rows, CELLS), F32),
            pltpu.VMEM((BLK + 1, 32, CELLS), F32),
            pltpu.VMEM((BLK + 1, 32, CELLS), F32),
            pltpu.VMEM((BLK + 1, 32, CELLS), BF16),
            pltpu.VMEM((BLK + 1, 32, CELLS), BF16),
            pltpu.VMEM((peers, CAP * CELLS, CELLS), BF16),
            pltpu.VMEM((levels, CAP * CELLS, CELLS), BF16),
            pltpu.VMEM((BLK, CELLS, CELLS), BF16),
            pltpu.SMEM((1, BLK), jnp.int32),
            pltpu.SMEM((CAP, peers), jnp.int32),
            pltpu.SMEM((CAP, peers), jnp.int32),
            pltpu.SMEM((1, peers), jnp.int32),
            pltpu.SMEM((CAP, levels), jnp.int32),
            pltpu.SMEM((CAP, levels), jnp.int32),
            pltpu.SMEM((1, levels), jnp.int32),
        ],
    )(
        flat,
        own_src,
        own_weight[0],
        send_block[0, 0].T,
        send_target[0, 0].T,
        send_count[0],
        send_weight.reshape(peers, CAP * CELLS, CELLS),
        left_block[0, 0].T,
        left_target[0, 0].T,
        left_count[0],
        left_weight.reshape(levels, CAP * CELLS, CELLS),
    )
    sends = {"dev": send_dev, "level": send_lev}
    early = exchange(sends[ORDER[0]], ORDER[0])
    second = sends[ORDER[1]]
    second, base = pl.pallas_call(
        relay_kernel,
        name="relay",
        in_specs=[vmem] * 3,
        out_specs=[vmem] * 2,
        out_shape=[pltpu.VMEM(second.shape, BF16), pltpu.VMEM((rows, CELLS), F32)],
        input_output_aliases={2: 0},
    )(early, in_vmem(own), in_vmem(second))
    late = exchange(second, ORDER[1])
    remapped, totals = pl.pallas_call(
        final_kernel,
        name="final",
        in_specs=[vmem, vmem, vmem],
        out_specs=[vmem, vmem],
        out_shape=[
            jax.ShapeDtypeStruct((rows, CELLS), F32),
            jax.ShapeDtypeStruct((1, COMP), F32),
        ],
    )(early, late, in_vmem(base))
    remapped = jnp.transpose(remapped.reshape(COMP, BLK, CELLS), (1, 0, 2))
    return (remapped[None], totals.reshape(COMP))


def solution(mesh):
    return jax.shard_map(
        body,
        mesh=mesh,
        in_specs=(
            P("level", "dev", None, None),
            P("level", "dev"),
            P("level", "dev", None, None),
            P("level", "dev", None, None),
            P("level", "dev", None, None),
            P("level", "dev", None),
            P("level", "dev", None, None, None, None),
            P("level", "dev", None, None),
            P("level", "dev", None, None),
            P("level", "dev", None),
            P("level", "dev", None, None, None, None),
        ),
        out_specs=(P("level", "dev", None, None), P()),
        check_vma=False,
    )
```

```python
import functools

import jax
import jax.numpy as jnp
from jax import lax
from jax.experimental import pallas as pl
from jax.experimental.pallas import tpu as pltpu
from jax.sharding import PartitionSpec as P

GROUPS = {
    "dev": [21, 22, 23, 24, 25, 26, 27, 28, 29, 30, 31, 0, 1, 2, 3, 4, 5, 6, 7, 8, 9, 10, 11, 12, 13, 14, 15, 16, 17, 18, 19, 20],
    "level": [10, 0, 1, 2, 3, 15, 4, 14, 5, 13, 6, 12, 7, 11, 8, 9],
}
ORDER = ("dev", "level")
WAITING = 8
COMP = 12
CELLS = 128
BLK = 16
CAP = 2
ROWS = 26
PAIRS = ROWS // 2
GROUP = 4
PART = 32
W_CHUNKS = 2
F32 = jnp.float32
BF16 = jnp.bfloat16


def code_tile(t0, t1, slot):
    row = lax.broadcasted_iota(jnp.int32, (8, CELLS), 0)
    r = lax.broadcasted_iota(jnp.int32, (8, CELLS), 1) - slot * ROWS
    here = (row == 0) & (r >= 0) & (r < ROWS)
    second = r >= COMP
    comp = jnp.where(second, r - COMP, r)
    code = comp * BLK + jnp.where(second, t1, t0)
    code = jnp.where(r < CAP * COMP, code, 255)
    return jnp.where(here, code, 0).astype(F32)


def three_parts(total):
    row = lax.broadcasted_iota(jnp.int32, (8, CELLS), 0)
    full = jnp.broadcast_to(total, (8, CELLS))
    hi = full.astype(BF16).astype(F32)
    mid = (full - hi).astype(BF16).astype(F32)
    low = full - hi - mid
    parts = hi + pltpu.roll(mid, PART, 1) + pltpu.roll(low, 2 * PART, 1)
    return jnp.where(row == 1, parts, jnp.zeros_like(parts))


def sum_parts(row):
    full = jnp.broadcast_to(row, (8, CELLS))
    full = full + pltpu.roll(full, CELLS - PART, 1) + pltpu.roll(full, CELLS - 2 * PART, 1)
    lane = lax.broadcasted_iota(jnp.int32, (8, CELLS), 1)
    return jnp.where(lane < CAP * COMP, full, jnp.zeros_like(full))


def last_pair(recv, sl):
    return jnp.sum(recv[sl, PAIRS - 1].astype(F32), axis=0)


def terms_kernel(
    fields,
    own_src,
    own_w,
    send_blk,
    send_tgt,
    send_cnt,
    send_w,
    left_blk,
    left_tgt,
    left_cnt,
    left_w,
    out_dev,
    out_lev,
    own_out,
    fld,
    first32,
    second32,
    first,
    second,
    wd,
    wl,
    wo,
    s_src,
    s_sblk,
    s_stgt,
    s_scnt,
    s_lblk,
    s_ltgt,
    s_lcnt,
    sems,
    wsems,
):
    peers = send_w.shape[0]
    levels = left_w.shape[0]
    small = []
    pairs = (
        (fields, fld),
        (own_src, s_src),
        (send_blk, s_sblk),
        (send_tgt, s_stgt),
        (send_cnt, s_scnt),
        (left_blk, s_lblk),
        (left_tgt, s_ltgt),
        (left_cnt, s_lcnt),
    )
    copy = pltpu.make_async_copy(fields, fld, sems.at[0])
    copy.start()
    small.append(copy)
    step = peers // W_CHUNKS
    left_copy = pltpu.make_async_copy(left_w, wl, wsems.at[W_CHUNKS])
    left_copy.start()
    own_copy = pltpu.make_async_copy(own_w, wo, wsems.at[W_CHUNKS + 1])
    own_copy.start()
    weights = []
    for n in range(W_CHUNKS):
        sl = pl.ds(n * step, step)
        copy = pltpu.make_async_copy(send_w.at[sl], wd.at[sl], wsems.at[n])
        copy.start()
        weights.append(copy)

    for n, (src, dst) in enumerate(pairs[1:], 1):
        copy = pltpu.make_async_copy(src, dst, sems.at[n])
        copy.start()
        small.append(copy)
    first32[...] = jnp.zeros(first32.shape, F32)
    second32[...] = jnp.zeros(second32.shape, F32)
    small[0].wait()
    for b in range(BLK):
        one = fld[pl.ds(b, COMP, stride=BLK), :]
        first32[b, 0:COMP, :] = one
        second32[b, COMP : 2 * COMP, :] = one
    first[...] = first32[...].astype(BF16)
    second[...] = second32[...].astype(BF16)
    for copy in small[1:]:
        copy.wait()

    def group_terms(out, blk, tgt, cnt, weight, axis):
        size = out.shape[0]
        here = lax.axis_index(axis)
        slot = jnp.int32(0)
        for n, member in enumerate(GROUPS[axis]):
            slot = jnp.where(here == member, n % GROUP, slot)

        def one(n, acc):
            live = cnt[0, n]
            b0 = jnp.where(live > 0, blk[0, n], BLK)
            b1 = jnp.where(live > 1, blk[1, n], BLK)
            lhs = jnp.concatenate([first[b0], second[b1]], axis=1)
            t = jnp.dot(lhs, weight[n], preferred_element_type=F32)
            to = GROUPS[axis].index(n)
            flat = out.reshape(size * ROWS, CELLS)
            codes = code_tile(tgt[0, n], tgt[1, n], slot)
            message = jnp.concatenate([t[0:24], codes], axis=0).astype(BF16)
            flat[to * ROWS : (to + 1) * ROWS, :] = message[0:ROWS]
            return acc + t[0:24]

        return one

    dev_step = group_terms(out_dev, s_sblk, s_stgt, s_scnt, wd, "dev")
    lev_step = group_terms(out_lev, s_lblk, s_ltgt, s_lcnt, wl, "level")
    acc = jnp.zeros((24, CELLS), F32)
    left_copy.wait()
    own_copy.wait()
    for level in range(levels):
        acc = lev_step(level, acc)
    own_acc = jnp.zeros((16, CELLS), F32)
    for b in range(BLK):
        t = jnp.dot(first[s_src[0, b], 0:16, :], wo[b], preferred_element_type=F32)
        own_out[pl.ds(b, COMP, stride=BLK), :] = t[0:COMP]
        own_acc = own_acc + t
    for n in range(W_CHUNKS):
        weights[n].wait()
        for peer in range(n * step, (n + 1) * step):
            acc = dev_step(peer, acc)
    acc = acc + jnp.concatenate([own_acc, jnp.zeros((8, CELLS), F32)], axis=0)
    row = lax.broadcasted_iota(jnp.int32, acc.shape, 0)
    lane = lax.broadcasted_iota(jnp.int32, acc.shape, 1)
    sums = jnp.where(row == lane, jnp.sum(acc, axis=1, keepdims=True), jnp.zeros_like(acc))
    sums = jnp.sum(sums, axis=0, keepdims=True)
    add_parts(out_dev if ORDER[0] == "dev" else out_lev, sums[0:1])


def scoped_terms(*refs):
    pl.run_scoped(
        functools.partial(terms_kernel, *refs),
        pltpu.SemaphoreType.DMA((8,)),
        pltpu.SemaphoreType.DMA((W_CHUNKS + 2,)),
    )


def add_parts(message, total):
    message[:, PAIRS - 1] += three_parts(total)[0:2].astype(BF16)[None]


def places_early():
    return lax.axis_index("level") < WAITING


def relay_kernel(recv, own, send_in, send_out, base):
    del send_in
    add_parts(send_out, sum_parts(last_pair(recv, slice(None))[1:2])[0:1])

    @pl.when(places_early())
    def _():
        base[...] = own[...] + placed(recv)

    @pl.when(jnp.logical_not(places_early()))
    def _():
        base[...] = own[...]


def placed(recv):
    peers = recv.shape[0]
    flat = recv.reshape(peers * ROWS, CELLS)
    row = lax.broadcasted_iota(jnp.int32, (COMP * BLK, CELLS), 0).astype(F32)
    total = jnp.zeros((COMP * BLK, CELLS), F32)
    for g in range(peers // GROUP):
        codes = last_pair(recv, slice(g * GROUP, (g + 1) * GROUP))[0:1]
        pick = jnp.where(row == codes, 1.0, 0.0).astype(BF16)[:, : GROUP * ROWS]
        data = flat[g * GROUP * ROWS : (g + 1) * GROUP * ROWS, :]
        total = total + jnp.dot(pick, data, preferred_element_type=F32)
    return total


def final_kernel(early, late, base, out, totals):
    out[...] = base[...] + placed(late)

    @pl.when(jnp.logical_not(places_early()))
    def _():
        out[...] += placed(early)

    both = sum_parts(last_pair(late, slice(None))[1:2])
    both = both + pltpu.roll(both, CELLS - COMP, 1)
    totals[...] = both[0:1, 0:COMP] * (1.0 / (CELLS * BLK))


def in_vmem(x):
    return pltpu.with_memory_space_constraint(x, pltpu.VMEM)


def exchange(message, axis):
    groups = [GROUPS[axis]]
    got = lax.all_to_all(in_vmem(message), axis, 0, 0, axis_index_groups=groups, tiled=True)
    return in_vmem(got)


def body(
    fields,
    own_src,
    own_weight,
    send_block,
    send_target,
    send_count,
    send_weight,
    left_block,
    left_target,
    left_count,
    left_weight,
):
    peers = send_weight.shape[2]
    levels = left_weight.shape[2]
    rows = COMP * BLK
    flat = jnp.transpose(fields[0], (1, 0, 2)).reshape(rows, CELLS)
    anywhere = pl.BlockSpec(memory_space=pl.ANY)
    vmem = pl.BlockSpec(memory_space=pltpu.VMEM)
    send_dev, send_lev, own = pl.pallas_call(
        scoped_terms,
        name="terms",
        in_specs=[anywhere] * 11,
        out_specs=[vmem] * 3,
        out_shape=[
            pltpu.VMEM((peers, PAIRS, 2, CELLS), BF16),
            pltpu.VMEM((levels, PAIRS, 2, CELLS), BF16),
            pltpu.VMEM((rows, CELLS), F32),
        ],
        scratch_shapes=[
            pltpu.VMEM((rows, CELLS), F32),
            pltpu.VMEM((BLK + 1, 32, CELLS), F32),
            pltpu.VMEM((BLK + 1, 32, CELLS), F32),
            pltpu.VMEM((BLK + 1, 32, CELLS), BF16),
            pltpu.VMEM((BLK + 1, 32, CELLS), BF16),
            pltpu.VMEM((peers, CAP * CELLS, CELLS), BF16),
            pltpu.VMEM((levels, CAP * CELLS, CELLS), BF16),
            pltpu.VMEM((BLK, CELLS, CELLS), BF16),
            pltpu.SMEM((1, BLK), jnp.int32),
            pltpu.SMEM((CAP, peers), jnp.int32),
            pltpu.SMEM((CAP, peers), jnp.int32),
            pltpu.SMEM((1, peers), jnp.int32),
            pltpu.SMEM((CAP, levels), jnp.int32),
            pltpu.SMEM((CAP, levels), jnp.int32),
            pltpu.SMEM((1, levels), jnp.int32),
        ],
    )(
        flat,
        own_src,
        own_weight[0],
        send_block[0, 0].T,
        send_target[0, 0].T,
        send_count[0],
        send_weight.reshape(peers, CAP * CELLS, CELLS),
        left_block[0, 0].T,
        left_target[0, 0].T,
        left_count[0],
        left_weight.reshape(levels, CAP * CELLS, CELLS),
    )
    sends = {"dev": send_dev, "level": send_lev}
    early = exchange(sends[ORDER[0]], ORDER[0])
    second = sends[ORDER[1]]
    second, base = pl.pallas_call(
        relay_kernel,
        name="relay",
        in_specs=[vmem] * 3,
        out_specs=[vmem] * 2,
        out_shape=[pltpu.VMEM(second.shape, BF16), pltpu.VMEM((rows, CELLS), F32)],
        input_output_aliases={2: 0},
    )(early, in_vmem(own), in_vmem(second))
    late = exchange(second, ORDER[1])
    remapped, totals = pl.pallas_call(
        final_kernel,
        name="final",
        in_specs=[vmem, vmem, vmem],
        out_specs=[vmem, vmem],
        out_shape=[
            jax.ShapeDtypeStruct((rows, CELLS), F32),
            jax.ShapeDtypeStruct((1, COMP), F32),
        ],
    )(early, late, in_vmem(base))
    remapped = jnp.transpose(remapped.reshape(COMP, BLK, CELLS), (1, 0, 2))
    return (remapped[None], totals.reshape(COMP))


def solution(mesh):
    return jax.shard_map(
        body,
        mesh=mesh,
        in_specs=(
            P("level", "dev", None, None),
            P("level", "dev"),
            P("level", "dev", None, None),
            P("level", "dev", None, None),
            P("level", "dev", None, None),
            P("level", "dev", None),
            P("level", "dev", None, None, None, None),
            P("level", "dev", None, None),
            P("level", "dev", None, None),
            P("level", "dev", None),
            P("level", "dev", None, None, None, None),
        ),
        out_specs=(P("level", "dev", None, None), P()),
        check_vma=False,
    )
```
